32 devices in a mesh: band: 16 (over z, y, core), chan: 2 (over x).
Axes of the slice: x: 2, y: 2, z: 4, core: 2. Of those that a mesh axis runs over, the one named last changes fastest.
Arguments:
- fine_features: bfloat16 [2, 192, 128, 512], P(None, 'chan', 'band'), may hold values from -100 to 100
- coarse_level: bfloat16 [2, 256, 64, 256], P(None, 'chan', 'band'), may hold values from -100 to 100
- lat_weight: bfloat16 [256, 192], P('chan'), may hold values from -0.4375 to 0.4375
- lat_gain: bfloat16 [256], P('chan'), may hold values from 0.099609375 to 1.8984375
- lat_shift: bfloat16 [256], P('chan'), may hold values from -3 to 3
- out_weight: bfloat16 [3, 3, 256, 256], P(None, None, 'chan'), may hold values from -0.125 to 0.125
- out_gain: bfloat16 [256], P('chan'), may hold values from 0.099609375 to 1.8984375
- out_shift: bfloat16 [256], P('chan'), may hold values from -3 to 3
- mask_weight: bfloat16 [256, 256], P('chan'), may hold values from -0.375 to 0.375
- mask_bias: bfloat16 [256], P('chan'), may hold values from -1.796875 to 1.796875
- queries: bfloat16 [200, 256], replicated, may hold values from -128 to 128
Outputs:
- log_probs: float32 [2, 200, 128, 512], P(None, None, ('band', 'chan'))
The draws below stay inside these ranges and needn't reach their ends.
All inputs are finite; a program needn't handle non-finite values.
Results may differ from the reference program's by a relative error of at most 0.0058.
Values may be sent and summed in bfloat16 or wider, within the bound.
A program may use at most 128 MiB of HBM per device.

```python
import jax
import jax.numpy as jnp
from jax import lax

D = 256
C4 = 192
QUERIES = 200
GROUPS = 32
IMAGES = 2
COLS = 512
H4 = 128


def banded_field(key, images, channels, height, width):
    key_noise = jax.random.fold_in(key, 0)
    key_rows = jax.random.fold_in(key, 1)
    key_cols = jax.random.fold_in(key, 2)
    key_offset = jax.random.fold_in(key, 4)
    positions = jnp.arange(height, dtype=jnp.float32) / max(height - 1, 1)
    ramp = 3.0 ** positions
    row_scale = ramp[None, :] * jnp.exp(jax.random.uniform(key_rows, (images, height), jnp.float32, -0.8, 0.8))
    col_scale = jnp.exp(jax.random.uniform(key_cols, (images, width), jnp.float32, -0.8, 0.8))
    scale = row_scale[:, None, :, None] * col_scale[:, None, None, :]
    offset = jax.random.uniform(key_offset, (images, channels, 1, 1), jnp.float32, -3.0, 3.0)
    noise = jax.random.truncated_normal(key_noise, -4.0, 4.0, (images, channels, height, width), jnp.float32)
    values = noise * scale + offset * ramp[None, None, :, None]
    return values


def draw_fine_features(key, part):
    return banded_field(jax.random.fold_in(key, 11), IMAGES, C4, H4, COLS).astype(jnp.bfloat16)


def draw_coarse_level(key, part):
    return banded_field(jax.random.fold_in(key, 12), IMAGES, D, H4 // 2, COLS // 2).astype(jnp.bfloat16)


def draw_queries(key, part):
    key_base = jax.random.fold_in(jax.random.fold_in(key, 13), 0)
    values = 0.25 * jax.random.truncated_normal(key_base, -4.0, 4.0, (QUERIES, D), jnp.float32)
    return values.astype(jnp.bfloat16)


def levels(own_key, extent, shards, smallest, high):
    factor_of = 1.0
    for axis_at, parts in shards:
        heights = jax.random.uniform(jax.random.fold_in(jax.random.fold_in(own_key, 6), axis_at), (parts,), jnp.float32, smallest / len(shards), high / len(shards))
        factor_of = factor_of * jnp.repeat(jnp.exp(heights), extent[axis_at] // parts).reshape((-1,) + (1,) * (len(extent) - 1 - axis_at))
    return factor_of


def bell_draw(stream_key, shape, spread, most, pieces=(), kind=jnp.bfloat16):
    values = jax.random.normal(stream_key, shape, jnp.float32) * spread
    if len(pieces) > 0:
        values = levels(stream_key, shape, pieces, -0.22, 0.18) * values
    return jnp.clip(values, min=-most, max=most).astype(kind)


def setup_inputs(seed: int = 0) -> dict:
    key_of = jax.random.split(jax.random.key(seed), 12)
    return {
        "fine_features": draw_fine_features(jax.random.fold_in(key_of[11], 71), 0),
        "coarse_level": draw_coarse_level(jax.random.fold_in(key_of[11], 71), 0),
        "lat_weight": bell_draw(key_of[2], (D, C4), C4 ** -0.5, 0.4375, ((0, 2),)),
        "lat_gain": jnp.clip(1.0 + 0.18 * jax.random.normal(key_of[3], (D,), jnp.float32), 0.099609375, 1.8984375).astype(jnp.bfloat16),
        "lat_shift": bell_draw(key_of[4], (D,), 0.5, 3.0, ((0, 2),)),
        "out_weight": bell_draw(key_of[5], (3, 3, D, D), (9 * D) ** -0.5, 0.125, ((2, 2),)),
        "out_gain": jnp.clip(1.0 + 0.18 * jax.random.normal(key_of[6], (D,), jnp.float32), 0.099609375, 1.8984375).astype(jnp.bfloat16),
        "out_shift": bell_draw(key_of[7], (D,), 0.5, 3.0, ((0, 2),)),
        "mask_weight": bell_draw(key_of[8], (D, D), D ** -0.5, 0.375, ((0, 2),)),
        "mask_bias": bell_draw(key_of[9], (D,), 0.3, 1.796875, ((0, 2),)),
        "queries": draw_queries(jax.random.fold_in(key_of[11], 71), 0),
    }


epsilon = 1e-05

def interp(padded, axis):
    length = padded.shape[axis] - 2
    before = lax.slice_in_dim(padded, 0, length, axis=axis)
    middle = lax.slice_in_dim(padded, 1, length + 1, axis=axis)
    after = lax.slice_in_dim(padded, 2, length + 2, axis=axis)
    even_part = 0.25 * before + 0.75 * middle
    odd_part = 0.75 * middle + 0.25 * after
    paired = jnp.stack([even_part, odd_part], axis + 1)
    new_shape = list(middle.shape)
    new_shape[axis] = 2 * length
    return paired.reshape(new_shape)

def group_norm(values, gain, shift, group_size):
    channels, height, width = values.shape
    blocks = values.reshape(channels // group_size, group_size * height * width)
    mean_value = lax.optimization_barrier(jnp.mean(blocks, axis=1, keepdims=True))
    deviation = blocks - mean_value
    variance = lax.optimization_barrier(jnp.mean(deviation * deviation, axis=1, keepdims=True))
    scaled = ((blocks - mean_value) * lax.rsqrt(variance + epsilon)).reshape(channels, height, width)
    return scaled * gain.astype(jnp.float32)[:, None, None] + shift.astype(jnp.float32)[:, None, None]

def reference(fine_features, coarse_level, lat_weight, lat_gain, lat_shift, out_weight, out_gain, out_shift, mask_weight, mask_bias, queries):
    group_size = D // GROUPS

    def one_image(pair):
        fine_image, coarse_image = pair
        lateral = jnp.dot(lat_weight, fine_image.reshape(C4, H4 * COLS), preferred_element_type=jnp.float32).reshape(D, H4, COLS)
        lat_normed = group_norm(lateral, lat_gain, lat_shift, group_size)
        extended = jnp.pad(coarse_image.astype(jnp.float32), ((0, 0), (1, 1), (1, 1)), mode='edge')
        upsampled = interp(interp(extended, 1), 2)
        joined = (lat_normed + upsampled).astype(jnp.bfloat16)
        padded = jnp.pad(joined, ((0, 0), (1, 1), (1, 1)))
        conv_out = jnp.zeros((D, H4 * COLS), jnp.float32)
        for row_tap in range(3):
            for col_tap in range(3):
                window = padded[:, row_tap:row_tap + H4, col_tap:col_tap + COLS].reshape(D, H4 * COLS)
                conv_out = conv_out + jnp.dot(out_weight[row_tap, col_tap], window, preferred_element_type=jnp.float32)
        conv_out = conv_out.reshape(D, H4, COLS)
        activated = jnp.maximum(group_norm(conv_out, out_gain, out_shift, group_size), 0.0).astype(jnp.bfloat16)
        features = jnp.dot(mask_weight, activated.reshape(D, H4 * COLS), preferred_element_type=jnp.float32)
        features = (features + mask_bias.astype(jnp.float32)[:, None]).astype(jnp.bfloat16)
        logits = jnp.dot(queries, features, preferred_element_type=jnp.float32)
        peak = lax.optimization_barrier(jnp.max(logits, axis=0, keepdims=True))
        shifted = logits - peak
        result = shifted - jnp.log(lax.optimization_barrier(jnp.sum(jnp.exp(shifted), axis=0, keepdims=True)))
        return result.reshape(QUERIES, H4, COLS)
    return lax.map(one_image, (fine_features, coarse_level))
```

```python
import functools
import math

import jax
import jax.numpy as jnp
from jax import lax
from jax.experimental import pallas as pl
from jax.experimental.pallas import tpu as pltpu
from jax.sharding import PartitionSpec as P

D = 256
GROUPS = 32
EPS = 1e-05
LANES = 128
MESH = pl.DeviceIdType.MESH
F32 = jnp.float32
BF16 = jnp.bfloat16


def wait_on(ref, sem):
    pltpu.make_async_copy(ref, ref, sem).wait()


def across(x, times):
    return jnp.concatenate([x] * times, axis=1)


def log_softmax_row(centred, scale, offset, mask, bias, queries):
    act = jnp.maximum(centred * scale + offset, 0.0).astype(BF16)
    mixed = jnp.dot(mask, act, preferred_element_type=F32)
    features = (mixed + bias).astype(BF16)
    logits = jnp.dot(queries, features, preferred_element_type=F32)
    shifted = logits - jnp.max(logits, axis=0, keepdims=True)
    norm = jnp.log(jnp.sum(jnp.exp(shifted), axis=0, keepdims=True))
    return shifted - norm


def kernel(
    bands, chans, pixel_count,
    fine, coarse, lat_in, par0, par1, par2, par3, par4, conv_in, mask_in, queries,
    done, last_conv, last_coef, mask_out,
    raw, craw, tmp, ctmp, fsend, csend,
    feats, level, ebuf, pbuf, wbuf, mbuf, wlat, wide, lat, cols_up, stacked, conv, rows_out,
    coef, stat1, stat2,
    r_sem, f_send, f_recv, fh_send, fh_recv, c_send, c_recv, ch_send, ch_recv,
    e_send, e_recv, w_send, w_recv, q_send, q_recv, s_send, s_recv, o_sem, k_sem,
):
    images, in_ch, band_rows, width = fine.shape
    c_ch, c_band = coarse.shape[1], coarse.shape[2]
    rows, c_rows = band_rows // chans, c_band // chans
    half_w = width // 2
    share = lat_in.shape[1]
    quad = math.gcd(bands, 4)
    quarter = share // quad
    gsize = D // GROUPS
    total = bands * chans
    times = width // LANES
    last = images - 1
    b = lax.axis_index("band")
    c = lax.axis_index("chan")
    me = b * chans + c
    sends = []

    barrier = pltpu.get_barrier_semaphore()

    def greet(k, carry):
        to = lax.rem(me + k, total)
        pl.semaphore_signal(
            barrier, inc=1, device_id=(to // chans, lax.rem(to, chans)), device_id_type=MESH)
        return carry

    lax.fori_loop(1, total, greet, 0)
    for n in range(images):
        pltpu.make_async_copy(fine.at[n], raw.at[n], r_sem.at[0, n]).start()
        pltpu.make_async_copy(coarse.at[n], craw.at[n], r_sem.at[1, n]).start()

    def send(src, dst, ssem, rsem, tb, tc, only=None):
        def remote():
            return pltpu.make_async_remote_copy(
                src_ref=src, dst_ref=dst, send_sem=ssem, recv_sem=rsem,
                device_id=(tb, tc), device_id_type=MESH,
            )

        if only is None:
            remote().start()
        else:
            @pl.when(only)
            def _():
                remote().start()
        sends.append((remote, only))

    def block(index, size):
        return pl.ds(pl.multiple_of(index * size, size), size)

    def gather(src, dst, ssem, rsem):
        pltpu.make_async_copy(src, dst.at[c], rsem.at[0]).start()
        for s in range(1, chans):
            send(src, dst.at[c], ssem.at[s], rsem.at[s], b, lax.rem(c + s, chans))

    spot = lax.rem(b, quad)

    def quarter_of(owner, part):
        return pl.ds(pl.multiple_of(owner * share + part * quarter, quarter), quarter)

    def weights_across(src, dst, ssem, rsem):
        for s in range(1, chans):
            send(
                src.at[:, pl.ds(pl.multiple_of(spot * quarter, quarter), quarter)],
                dst.at[:, quarter_of(c, spot)], ssem.at[s], rsem.at[s], b, lax.rem(c + s, chans),
            )
        pltpu.make_async_copy(src, dst.at[:, block(c, share)], rsem.at[0]).start()

    def weights_around(dst, rsem, ssem2, rsem2):
        for s in range(1, chans):
            wait_on(dst.at[:, pl.ds(0, quarter)], rsem.at[s])
            owner = lax.rem(c - s + chans, chans)
            piece = dst.at[:, quarter_of(owner, spot)]
            for m in range(1, quad):
                mate = b - spot + lax.rem(spot + m, quad)
                send(piece, piece, ssem2.at[s, m], rsem2.at[s, m], mate, c)

    def wait_weights(dst, rsem, rsem2):
        wait_on(dst.at[:, pl.ds(0, share)], rsem.at[0])
        for s in range(1, chans):
            for m in range(1, quad):
                wait_on(dst.at[:, pl.ds(0, quarter)], rsem2.at[s, m])

    def main_rows(src, dst, n, size, ch, ssem, rsem):
        for s in range(1, chans):
            t = lax.rem(c + s, chans)
            send(
                src.at[n, pl.ds(t * size, size)], dst.at[n, pl.ds(1, size), block(c, ch)],
                ssem.at[n, s], rsem.at[n, s], b, t,
            )

    def halo_rows(src, dst, n, size, ch, ssem, rsem):
        for s in range(chans):
            t = lax.rem(c + s, chans)
            k = (s + 1) % chans
            to = lax.rem(b * chans + t + 1, total)
            send(
                src.at[n, (t + 1) * size - 1], dst.at[n, 0, block(c, ch)],
                ssem.at[n, 0, s], rsem.at[n, 0, k], to // chans, lax.rem(to, chans),
                c == 0 if k == 0 else None,
            )
            k = (s - 1) % chans
            to = lax.rem(b * chans + t - 1 + total, total)
            send(
                src.at[n, t * size], dst.at[n, size + 1, block(c, ch)],
                ssem.at[n, 1, s], rsem.at[n, 1, k], to // chans, lax.rem(to, chans),
                c == chans - 1 if k == 0 else None,
            )

    def keep_own(src, dst, n, size, ch):
        own = block(c, ch)
        for i in range(size):
            dst[n, i + 1, own] = src[n, c * size + i]

        @pl.when(c > 0)
        def _():
            dst[n, 0, own] = src[n, c * size - 1]

        @pl.when(c < chans - 1)
        def _():
            dst[n, size + 1, own] = src[n, (c + 1) * size]

    def wait_main(dst, n, size, ch, rsem):
        for s in range(1, chans):
            wait_on(dst.at[n, pl.ds(1, size), pl.ds(0, ch)], rsem.at[n, s])

    def wait_halo(dst, n, size, ch, rsem):
        for side in range(2):
            for s in range(chans):
                def arrive():
                    wait_on(dst.at[n, side * (size + 1), pl.ds(0, ch)], rsem.at[n, side, s])

                if s == 0:
                    pl.when(c == (0, chans - 1)[side])(arrive)
                else:
                    arrive()

    def by_rows(src, dst, buf, n, pitch):
        channels, height, columns = src.shape[1], src.shape[2], src.shape[3]

        def lanes(k, carry):
            col = pl.ds(pl.multiple_of(k * LANES, LANES), LANES)
            for ch in range(channels):
                buf[pl.ds(ch * pitch, height), :] = src[n, ch, :, col].astype(F32)
            for r in range(height):
                dst[n, r, :, col] = buf[pl.ds(r, channels, stride=pitch), :].astype(BF16)
            return carry

        lax.fori_loop(0, columns // LANES, lanes, 0)

    def fine_rows(n):
        pltpu.make_async_copy(fine.at[n], raw.at[n], r_sem.at[0, n]).wait()
        by_rows(raw, fsend, tmp, n, tmp.shape[0] // in_ch)

    def coarse_rows(n):
        pltpu.make_async_copy(coarse.at[n], craw.at[n], r_sem.at[1, n]).wait()
        by_rows(craw, csend, ctmp, n, ctmp.shape[0] // c_ch)

    fine_rows(0)
    pl.semaphore_wait(barrier, total - 1)
    gather(lat_in, ebuf, e_send.at[0], e_recv.at[0])
    for k, par in enumerate((par0, par1, par2, par3, par4)):
        gather(par, pbuf.at[k], e_send.at[k + 1], e_recv.at[k + 1])
    for n in range(images):
        if n > 0:
            fine_rows(n)
        main_rows(fsend, feats, n, rows, in_ch, f_send, f_recv)
    weights_across(conv_in, wbuf, w_send.at[0], w_recv.at[0])
    for n in range(images):
        coarse_rows(n)
        halo_rows(fsend, feats, n, rows, in_ch, fh_send, fh_recv)
        main_rows(csend, level, n, c_rows, c_ch, c_send, c_recv)
        halo_rows(csend, level, n, c_rows, c_ch, ch_send, ch_recv)
        if n == 0:
            weights_across(mask_in, mbuf, w_send.at[1], w_recv.at[1])
    for n in range(images):
        keep_own(fsend, feats, n, rows, in_ch)
        keep_own(csend, level, n, c_rows, c_ch)

    local_count = float(gsize * rows * width)
    lane = lax.broadcasted_iota(jnp.int32, (D, LANES), 1)
    group = lax.broadcasted_iota(jnp.int32, (D, LANES), 0) // gsize

    def fold(x):
        acc = x[:, 0:LANES]
        for k in range(1, times):
            acc = acc + x[:, k * LANES:(k + 1) * LANES]
        return acc

    def to_row(x, slot):
        s = jnp.sum(x, axis=1, keepdims=True)
        return jnp.sum(jnp.where(lane == group + slot * GROUPS, s, 0.0), axis=0, keepdims=True)

    def from_row(row, slot):
        spread = jnp.where(lane == group + slot * GROUPS, row, 0.0)
        return jnp.sum(spread, axis=1, keepdims=True)

    def first_shift(y):
        mean = from_row(to_row(fold(y), 0), 0) / float(gsize * width)
        return jnp.broadcast_to(mean, (D, LANES))

    def stat_rows(s1, s2, shift, slot, slots):
        a = to_row(s1, slot)
        m2 = to_row(s2, slot) - a * a / local_count
        here = lax.broadcasted_iota(jnp.int32, (1, LANES), 1) // GROUPS == slot
        m2 = jnp.where(here, m2, 0.0)
        own = jnp.sum(
            jnp.where(lane == group + slot * GROUPS, shift, 0.0), axis=0, keepdims=True)
        s = a + own * (local_count / gsize)
        return s + pltpu.roll(m2, slots * GROUPS, 1)

    def exchange(row, buf, which):
        buf[0] = row

        def one(k, carry):
            to = lax.rem(me + k, total)
            pltpu.make_async_remote_copy(
                src_ref=buf.at[0], dst_ref=buf.at[k],
                send_sem=s_send.at[which], recv_sem=s_recv.at[which],
                device_id=(to // chans, lax.rem(to, chans)), device_id_type=MESH,
            ).start()
            return carry

        lax.fori_loop(1, total, one, 0)

    def combined(buf, which, slots):
        wait_on(buf.at[pl.ds(1, total - 1)], s_recv.at[which])
        parts = buf[...]
        sums = jnp.sum(parts, axis=0)
        mean = sums / pixel_count
        off = parts / local_count - mean[None]
        m2 = pltpu.roll(sums, LANES - slots * GROUPS, 1)
        var = (m2 + local_count * jnp.sum(off * off, axis=0)) / pixel_count
        inv = lax.rsqrt(var + EPS)
        return [(from_row(mean, n), from_row(inv, n)) for n in range(slots)]

    for k in range(6):
        for s in range(chans):
            wait_on((pbuf.at[k - 1] if k else ebuf).at[0], e_recv.at[k, s])
    square = (
        lax.broadcasted_iota(jnp.int32, (share, share), 0)
        == lax.broadcasted_iota(jnp.int32, (share, share), 1)
    )

    def column(k):
        return jnp.concatenate([
            jnp.sum(jnp.where(
                square, jnp.broadcast_to(pbuf[k, s].astype(F32), (share, share)), 0.0,
            ), axis=1, keepdims=True)
            for s in range(chans)
        ], axis=0)

    lat_gain, lat_shift, out_gain, out_shift, bias = (column(k) for k in range(5))
    for s in range(chans):
        wlat[s * share:(s + 1) * share, :] = ebuf[s].astype(F32).T.astype(BF16)

    def lateral(features):
        return jnp.dot(wlat[...], features, preferred_element_type=F32)

    SHIFT, SCALE, OFFSET, S1, S2 = range(5)

    def centre_first(y, slot):
        coef[slot, SHIFT] = first_shift(y)
        coef[slot, S1] = jnp.zeros((D, LANES), F32)
        coef[slot, S2] = jnp.zeros((D, LANES), F32)

    def centre(y, slot):
        d = y - across(coef[slot, SHIFT], times)
        coef[slot, S1] = coef[slot, S1] + fold(d)
        coef[slot, S2] = coef[slot, S2] + fold(d * d)
        return d

    def set_norm(slot, mean, inv, gain, shift):
        scale = inv * gain
        coef[slot, SCALE] = jnp.broadcast_to(scale, (D, LANES))
        centred = jnp.broadcast_to(mean, (D, LANES)) - coef[slot, SHIFT]
        coef[slot, OFFSET] = shift - centred * scale

    row1 = jnp.zeros((1, LANES), F32)
    for n in range(images):
        wait_main(feats, n, rows, in_ch, f_recv)
        y = lateral(feats[n, 1])
        centre_first(y, n)
        lat[n, 1] = centre(y, n)

        def step(r, carry, n=n):
            lat[n, r + 1] = centre(lateral(feats[n, r + 1]), n)
            return carry

        lax.fori_loop(1, rows, step, 0)
        row1 = row1 + stat_rows(coef[n, S1], coef[n, S2], coef[n, SHIFT], n, images)
    exchange(row1, stat1, 0)
    weights_around(wbuf, w_recv.at[0], q_send.at[0], q_recv.at[0])

    src_col = lax.broadcasted_iota(jnp.int32, (half_w, width), 0)
    dst_col = lax.broadcasted_iota(jnp.int32, (half_w, width), 1)
    half = dst_col // 2
    near = jnp.where(src_col == half, 0.75, 0.0)
    other = jnp.clip(jnp.where(dst_col - 2 * half == 0, half - 1, half + 1), 0, half_w - 1)
    up = (near + jnp.where(src_col == other, 0.25, 0.0)).astype(BF16)
    lane_w = lax.broadcasted_iota(jnp.int32, (D, width), 1)

    for n in range(images):
        wait_halo(feats, n, rows, in_ch, fh_recv)
        for j in (0, rows + 1):
            lat[n, j] = lateral(feats[n, j]) - across(coef[n, SHIFT], times)
        if n == 0:
            norms = combined(stat1, 0, images)
            for m in range(images):
                set_norm(m, norms[m][0], norms[m][1], lat_gain, lat_shift)
        wait_main(level, n, c_rows, c_ch, c_recv)
        wait_halo(level, n, c_rows, c_ch, ch_recv)

        def widen(k, carry, n=n):
            cols_up[k] = jnp.dot(level[n, k], up, preferred_element_type=F32)
            return carry

        lax.fori_loop(0, c_rows + 2, widen, 0)

        @pl.when(me == 0)
        def _():
            cols_up[0] = cols_up[1]

        @pl.when(me == total - 1)
        def _():
            cols_up[c_rows + 1] = cols_up[c_rows]

        def join(j, carry, n=n):
            k = j // 2
            even = j - 2 * k == 0
            w0 = jnp.where(even, 0.75, 0.25)
            w1 = jnp.where(even, 0.25, 0.75)
            upsampled = w0 * cols_up[k] + w1 * cols_up[k + 1]
            joined = (
                lat[n, j] * across(coef[n, SCALE], times)
                + across(coef[n, OFFSET], times) + upsampled)
            inside = jnp.logical_and(me * rows + j >= 1, me * rows + j <= total * rows)
            joined = jnp.where(inside, joined, 0.0)
            left = jnp.where(lane_w == 0, 0.0, pltpu.roll(joined, 1, 1))
            right = jnp.where(lane_w == width - 1, 0.0, pltpu.roll(joined, width - 1, 1))
            base = pl.multiple_of(j * 3 * D, D)
            stacked[pl.ds(base, D)] = left.astype(BF16)
            stacked[pl.ds(base + D, D)] = joined.astype(BF16)
            stacked[pl.ds(base + 2 * D, D)] = right.astype(BF16)
            return carry

        lax.fori_loop(0, rows + 2, join, 0)
        if n == 0:
            wait_weights(wbuf, w_recv.at[0], q_recv.at[0])
            for k in range(9):
                wide[:, k * D:(k + 1) * D] = wbuf[k]

        def convolve(r):
            base = pl.multiple_of(r * 3 * D, D)
            return jnp.dot(wide[...], stacked[pl.ds(base, 9 * D)], preferred_element_type=F32)

        slot = images + n

        def keep(r, y, n=n, slot=slot):
            conv[n, r] = centre(y, slot)
            if n == last:
                pltpu.make_async_copy(conv.at[n, r], last_conv.at[r], k_sem.at[r]).start()

        y = convolve(0)
        centre_first(y, slot)
        keep(0, y)

        def more(r, carry):
            keep(r, convolve(r))
            return carry

        lax.fori_loop(1, rows, more, 0)
        exchange(
            stat_rows(coef[slot, S1], coef[slot, S2], coef[slot, SHIFT], 0, 1), stat2.at[n], 1 + n)
        if n == 0:
            weights_around(mbuf, w_recv.at[1], q_send.at[1], q_recv.at[1])

    wait_weights(mbuf, w_recv.at[1], q_recv.at[1])
    pltpu.make_async_copy(mbuf.at[0], mask_out, k_sem.at[rows]).start()
    for n in range(last):
        slot = images + n
        mean, inv = combined(stat2.at[n], 1 + n, 1)[0]
        set_norm(slot, mean, inv, out_gain, out_shift)

        def finish(r, carry, n=n, slot=slot):
            rows_out[n, r] = log_softmax_row(
                conv[n, r], across(coef[slot, SCALE], times), across(coef[slot, OFFSET], times),
                mbuf[0], bias, queries[...])
            pltpu.make_async_copy(rows_out.at[n, r], done.at[n, :, r], o_sem.at[n, r]).start()
            return carry

        lax.fori_loop(0, rows, finish, 0)

    slot = images + last
    mean, inv = combined(stat2.at[last], 1 + last, 1)[0]
    set_norm(slot, mean, inv, out_gain, out_shift)
    coef[slot, SHIFT] = jnp.broadcast_to(bias, (D, LANES))
    pltpu.make_async_copy(
        coef.at[slot, pl.ds(0, 3)], last_coef, k_sem.at[rows + 1]).start()

    for which in range(1 + images):
        buf = stat1 if which == 0 else stat2.at[which - 1]
        wait_on(buf.at[pl.ds(1, total - 1)], s_send.at[which])
    for remote, only in sends:
        if only is None:
            remote().wait_send()
        else:
            @pl.when(only)
            def _():
                remote().wait_send()
    for n in range(last):
        for r in range(rows):
            pltpu.make_async_copy(rows_out.at[n, r], done.at[n, :, r], o_sem.at[n, r]).wait()
    for r in range(rows):
        pltpu.make_async_copy(conv.at[last, r], last_conv.at[r], k_sem.at[r]).wait()
    pltpu.make_async_copy(mbuf.at[0], mask_out, k_sem.at[rows]).wait()
    pltpu.make_async_copy(coef.at[slot, pl.ds(0, 3)], last_coef, k_sem.at[rows + 1]).wait()


def tail(
    done, conv, coef_in, mask_in, queries_in, out,
    rows_in, whole, rows_out, coef, mask, queries, c_sem, d_sem, o_sem, i_sem,
):
    rows, _, width = conv.shape
    last = out.shape[0] - 1
    times = width // LANES
    small = [(coef_in, coef), (mask_in, mask), (queries_in, queries)]
    for k, (src, dst) in enumerate(small):
        pltpu.make_async_copy(src, dst, i_sem.at[k]).start()
    for r in range(rows):
        pltpu.make_async_copy(conv.at[r], rows_in.at[r], c_sem.at[r]).start()
    for n in range(last):
        pltpu.make_async_copy(done.at[n], whole.at[n], d_sem.at[0, n]).start()
    for k, (src, dst) in enumerate(small):
        pltpu.make_async_copy(src, dst, i_sem.at[k]).wait()
    for r in range(rows):
        pltpu.make_async_copy(conv.at[r], rows_in.at[r], c_sem.at[r]).wait()
        rows_out[r] = log_softmax_row(
            rows_in[r], across(coef[1], times), across(coef[2], times),
            mask[...], across(coef[0], times), queries[...])
        pltpu.make_async_copy(rows_out.at[r], out.at[last, :, r], o_sem.at[r]).start()
        if r == 0:
            for n in range(last):
                pltpu.make_async_copy(done.at[n], whole.at[n], d_sem.at[0, n]).wait()
                pltpu.make_async_copy(whole.at[n], out.at[n], d_sem.at[1, n]).start()
    for n in range(last):
        pltpu.make_async_copy(whole.at[n], out.at[n], d_sem.at[1, n]).wait()
    for r in range(rows):
        pltpu.make_async_copy(rows_out.at[r], out.at[last, :, r], o_sem.at[r]).wait()


def banded(
    bands, chans,
    fine, coarse, lat_weight, lat_gain, lat_shift, out_weight, out_gain, out_shift,
    mask_weight, mask_bias, queries,
):
    images, in_ch, band_rows, width = fine.shape
    share = lat_weight.shape[0]
    c_ch, c_band = coarse.shape[1], coarse.shape[2]
    rows, c_rows = band_rows // chans, c_band // chans
    query_count = queries.shape[0]
    pixel_count = float(D // GROUPS * band_rows * bands * width)
    params = [v.reshape(1, share) for v in (lat_gain, lat_shift, out_gain, out_shift, mask_bias)]
    anywhere = pl.BlockSpec(memory_space=pl.ANY)
    vmem = pl.BlockSpec(memory_space=pltpu.VMEM)
    dma = pltpu.SemaphoreType.DMA
    before = max(images - 1, 1)
    pitch = band_rows + 1 - band_rows % 2
    c_pitch = c_band
    done, conv, coef, mask = pl.pallas_call(
        functools.partial(kernel, bands, chans, pixel_count),
        out_shape=[
            jax.ShapeDtypeStruct((before, query_count, rows, width), F32),
            jax.ShapeDtypeStruct((rows, D, width), F32),
            jax.ShapeDtypeStruct((3, D, LANES), F32),
            jax.ShapeDtypeStruct((D, D), BF16),
        ],
        in_specs=[anywhere] * 10 + [vmem],
        out_specs=[anywhere] * 4,
        scratch_shapes=[
            pltpu.VMEM((images, in_ch, band_rows, width), BF16),
            pltpu.VMEM((images, c_ch, c_band, width // 2), BF16),
            pltpu.VMEM((in_ch * pitch, LANES), F32),
            pltpu.VMEM((c_ch * c_pitch, LANES), F32),
            pltpu.VMEM((images, band_rows, in_ch, width), BF16),
            pltpu.VMEM((images, c_band, c_ch, width // 2), BF16),
            pltpu.VMEM((images, rows + 2, chans * in_ch, width), BF16),
            pltpu.VMEM((images, c_rows + 2, chans * c_ch, width // 2), BF16),
            pltpu.VMEM((chans, chans * in_ch, share), BF16),
            pltpu.VMEM((5, chans, 1, share), BF16),
            pltpu.VMEM((9, D, D), BF16),
            pltpu.VMEM((1, D, D), BF16),
            pltpu.VMEM((D, chans * in_ch), BF16),
            pltpu.VMEM((D, 9 * D), BF16),
            pltpu.VMEM((images, rows + 2, D, width), F32),
            pltpu.VMEM((c_rows + 2, D, width), F32),
            pltpu.VMEM(((rows + 2) * 3 * D, width), BF16),
            pltpu.VMEM((images, rows, D, width), F32),
            pltpu.VMEM((before, rows, query_count, width), F32),
            pltpu.VMEM((2 * images, 5, D, LANES), F32),
            pltpu.VMEM((bands * chans, 1, LANES), F32),
            pltpu.VMEM((images, bands * chans, 1, LANES), F32),
            dma((2, images)),
            dma((images, chans)), dma((images, chans)),
            dma((images, 2, chans)), dma((images, 2, chans)),
            dma((images, chans)), dma((images, chans)),
            dma((images, 2, chans)), dma((images, 2, chans)),
            dma((6, chans)), dma((6, chans)), dma((2, chans)), dma((2, chans)),
            dma((2, chans, 4)), dma((2, chans, 4)),
            dma((1 + images,)), dma((1 + images,)),
            dma((before, rows)), dma((rows + 2,)),
        ],
        compiler_params=pltpu.CompilerParams(
            has_side_effects=True, collective_id=0, vmem_limit_bytes=60 * 1024 * 1024),
    )(
        fine, coarse, lat_weight.T, *params, out_weight.reshape(9, share, D), mask_weight[None],
        queries,
    )
    return pl.pallas_call(
        tail,
        out_shape=jax.ShapeDtypeStruct((images, query_count, rows, width), F32),
        in_specs=[anywhere] * 5,
        out_specs=anywhere,
        scratch_shapes=[
            pltpu.VMEM((rows, D, width), F32),
            pltpu.VMEM((before, query_count, rows, width), F32),
            pltpu.VMEM((rows, query_count, width), F32),
            pltpu.VMEM((3, D, LANES), F32),
            pltpu.VMEM((D, D), BF16),
            pltpu.VMEM((query_count, D), BF16),
            dma((rows,)), dma((2, before)), dma((rows,)), dma((3,)),
        ],
        compiler_params=pltpu.CompilerParams(vmem_limit_bytes=60 * 1024 * 1024),
    )(done, conv, coef, mask, queries)


def gathered(
    bands, chans,
    fine, coarse, lat_weight, lat_gain, lat_shift, out_weight, out_gain, out_shift,
    mask_weight, mask_bias, queries,
):
    def whole(x, axis):
        return lax.all_gather(x, "chan", axis=axis, tiled=True)

    fine, coarse = whole(fine, 1), whole(coarse, 1)
    lat_weight, mask_weight = whole(lat_weight, 0), whole(mask_weight, 0)
    out_weight = whole(out_weight, 2)
    lat_gain, lat_shift, out_gain, out_shift, mask_bias = (
        whole(v, 0).astype(F32)[None, :, None, None]
        for v in (lat_gain, lat_shift, out_gain, out_shift, mask_bias))
    images, _, band_rows, width = fine.shape
    c_band, half_w = coarse.shape[2], coarse.shape[3]
    rows = band_rows // chans
    b = lax.axis_index("band")
    count = float(D // GROUPS * band_rows * bands * width)

    def norm(x, gain, shift, over):
        grouped = x.reshape(images, GROUPS, -1)
        mean = lax.psum(jnp.sum(grouped, axis=2), over) / count
        off = grouped - mean[:, :, None]
        var = lax.psum(jnp.sum(off * off, axis=2), over) / count
        y = (off * lax.rsqrt(var + EPS)[:, :, None]).reshape(x.shape)
        return y * gain + shift

    def with_border(x, clamp):
        n = x.shape[2]
        down = [(k, (k + 1) % bands) for k in range(bands)]
        upward = [((k + 1) % bands, k) for k in range(bands)]
        above = lax.ppermute(x[:, :, n - 1:], "band", down)
        below = lax.ppermute(x[:, :, :1], "band", upward)
        above = jnp.where(b == 0, x[:, :, :1] if clamp else jnp.zeros_like(above), above)
        below = jnp.where(
            b == bands - 1, x[:, :, n - 1:] if clamp else jnp.zeros_like(below), below)
        return jnp.concatenate([above, x, below], axis=2)

    def doubled(x, axis):
        n = x.shape[axis] - 2
        low, mid, high = (lax.slice_in_dim(x, k, k + n, axis=axis) for k in range(3))
        pair = jnp.stack([0.25 * low + 0.75 * mid, 0.75 * mid + 0.25 * high], axis + 1)
        return pair.reshape(x.shape[:axis] + (2 * n,) + x.shape[axis + 1:])

    def mix(w, x):
        return jnp.einsum("oi,nirc->norc", w, x, preferred_element_type=F32)

    lateral = norm(mix(lat_weight, fine), lat_gain, lat_shift, "band")
    tall = doubled(with_border(coarse, True).astype(F32), 2)
    upsampled = doubled(jnp.pad(tall, ((0, 0), (0, 0), (0, 0), (1, 1)), mode="edge"), 3)
    joined = (lateral + upsampled).astype(BF16)
    padded = lax.dynamic_slice_in_dim(
        with_border(joined, False), lax.axis_index("chan") * rows, rows + 2, axis=2)
    padded = jnp.pad(padded, ((0, 0), (0, 0), (0, 0), (1, 1)))
    conv = sum(
        mix(out_weight[a, t], padded[:, :, a:a + rows, t:t + width])
        for a in range(3) for t in range(3))
    act = jnp.maximum(norm(conv, out_gain, out_shift, ("band", "chan")), 0.0).astype(BF16)
    features = (mix(mask_weight, act) + mask_bias).astype(BF16)
    logits = mix(queries, features)
    shifted = logits - jnp.max(logits, axis=1, keepdims=True)
    return shifted - jnp.log(jnp.sum(jnp.exp(shifted), axis=1, keepdims=True))


def per_device(bands, chans, fine, coarse, *rest):
    thick = coarse.shape[2] % chans == 0 and fine.shape[2] == 2 * coarse.shape[2]
    return (banded if thick else gathered)(bands, chans, fine, coarse, *rest)


def solution(mesh):
    return jax.shard_map(
        functools.partial(per_device, mesh.shape["band"], mesh.shape["chan"]),
        mesh=mesh,
        in_specs=(
            P(None, "chan", "band", None),
            P(None, "chan", "band", None),
            P("chan", None),
            P("chan"),
            P("chan"),
            P(None, None, "chan", None),
            P("chan"),
            P("chan"),
            P("chan", None),
            P("chan"),
            P(),
        ),
        out_specs=P(None, None, ("band", "chan"), None),
        check_vma=False,
    )
```

```python
import functools
import math

import jax
import jax.numpy as jnp
from jax import lax
from jax.experimental import pallas as pl
from jax.experimental.pallas import tpu as pltpu
from jax.sharding import PartitionSpec as P

D = 256
GROUPS = 32
EPS = 1e-05
LANES = 128
MESH = pl.DeviceIdType.MESH
F32 = jnp.float32
BF16 = jnp.bfloat16


def wait_on(ref, sem):
    pltpu.make_async_copy(ref, ref, sem).wait()


def across(x, times):
    return jnp.concatenate([x] * times, axis=1)


def log_softmax_row(centred, scale, offset, mask, bias, queries):
    act = jnp.maximum(centred * scale + offset, 0.0).astype(BF16)
    mixed = jnp.dot(mask, act, preferred_element_type=F32)
    features = (mixed + bias).astype(BF16)
    logits = jnp.dot(queries, features, preferred_element_type=F32)
    shifted = logits - jnp.max(logits, axis=0, keepdims=True)
    norm = jnp.log(jnp.sum(jnp.exp(shifted), axis=0, keepdims=True))
    return shifted - norm


def kernel(
    bands, chans, pixel_count,
    fine, coarse, lat_in, par0, par1, par2, par3, par4, conv_in, mask_in, queries,
    done, last_conv, last_coef, mask_out,
    raw, craw, tmp, ctmp, fsend, csend, up,
    feats, level, ebuf, pbuf, wbuf, mbuf, wlat, wide, lat, cols_up, stacked, conv, rows_out,
    coef, stat1, stat2,
    r_sem, f_send, f_recv, fh_send, fh_recv, c_send, c_recv, ch_send, ch_recv,
    e_send, e_recv, w_send, w_recv, q_send, q_recv, s_send, s_recv, o_sem, k_sem,
):
    images, in_ch, band_rows, width = fine.shape
    c_ch, c_band = coarse.shape[1], coarse.shape[2]
    rows, c_rows = band_rows // chans, c_band // chans
    half_w = width // 2
    share = lat_in.shape[1]
    quad = math.gcd(bands, 4)
    quarter = share // quad
    gsize = D // GROUPS
    total = bands * chans
    times = width // LANES
    last = images - 1
    b = lax.axis_index("band")
    c = lax.axis_index("chan")
    me = b * chans + c
    sends = []

    barrier = pltpu.get_barrier_semaphore()

    def greet(k, carry):
        to = lax.rem(me + k, total)
        pl.semaphore_signal(
            barrier, inc=1, device_id=(to // chans, lax.rem(to, chans)), device_id_type=MESH)
        return carry

    lax.fori_loop(1, total, greet, 0)
    for n in range(images):
        pltpu.make_async_copy(fine.at[n], raw.at[n], r_sem.at[0, n]).start()
        pltpu.make_async_copy(coarse.at[n], craw.at[n], r_sem.at[1, n]).start()

    def send(src, dst, ssem, rsem, tb, tc, only=None):
        def remote():
            return pltpu.make_async_remote_copy(
                src_ref=src, dst_ref=dst, send_sem=ssem, recv_sem=rsem,
                device_id=(tb, tc), device_id_type=MESH,
            )

        if only is None:
            remote().start()
        else:
            @pl.when(only)
            def _():
                remote().start()
        sends.append((remote, only))

    def block(index, size):
        return pl.ds(pl.multiple_of(index * size, size), size)

    def gather(src, dst, ssem, rsem):
        pltpu.make_async_copy(src, dst.at[c], rsem.at[0]).start()
        for s in range(1, chans):
            send(src, dst.at[c], ssem.at[s], rsem.at[s], b, lax.rem(c + s, chans))

    spot = lax.rem(b, quad)

    def quarter_of(owner, part):
        return pl.ds(pl.multiple_of(owner * share + part * quarter, quarter), quarter)

    def weights_across(src, dst, ssem, rsem):
        for s in range(1, chans):
            send(
                src.at[:, pl.ds(pl.multiple_of(spot * quarter, quarter), quarter)],
                dst.at[:, quarter_of(c, spot)], ssem.at[s], rsem.at[s], b, lax.rem(c + s, chans),
            )
        pltpu.make_async_copy(src, dst.at[:, block(c, share)], rsem.at[0]).start()

    def weights_around(dst, rsem, ssem2, rsem2):
        for s in range(1, chans):
            wait_on(dst.at[:, pl.ds(0, quarter)], rsem.at[s])
            owner = lax.rem(c - s + chans, chans)
            piece = dst.at[:, quarter_of(owner, spot)]
            for m in range(1, quad):
                mate = b - spot + lax.rem(spot + m, quad)
                send(piece, piece, ssem2.at[s, m], rsem2.at[s, m], mate, c)

    def wait_weights(dst, rsem, rsem2):
        wait_on(dst.at[:, pl.ds(0, share)], rsem.at[0])
        for s in range(1, chans):
            for m in range(1, quad):
                wait_on(dst.at[:, pl.ds(0, quarter)], rsem2.at[s, m])

    def main_rows(src, dst, n, size, ch, ssem, rsem):
        for s in range(1, chans):
            t = lax.rem(c + s, chans)
            send(
                src.at[n, pl.ds(t * size, size)], dst.at[n, pl.ds(1, size), block(c, ch)],
                ssem.at[n, s], rsem.at[n, s], b, t,
            )

    def top_rows(src, dst, n, size, ch, ssem, rsem):
        for s in range(chans):
            t = lax.rem(c + s, chans)
            k = (s + 1) % chans
            to = lax.rem(b * chans + t + 1, total)
            send(
                src.at[n, (t + 1) * size - 1], dst.at[n, 0, block(c, ch)],
                ssem.at[n, 0, s], rsem.at[n, 0, k], to // chans, lax.rem(to, chans),
                c == 0 if k == 0 else None,
            )

    def bottom_rows(src, dst, n, size, ch, ssem, rsem):
        for s in range(chans):
            t = lax.rem(c + s, chans)
            k = (s - 1) % chans
            to = lax.rem(b * chans + t - 1 + total, total)
            send(
                src.at[n, t * size], dst.at[n, size + 1, block(c, ch)],
                ssem.at[n, 1, s], rsem.at[n, 1, k], to // chans, lax.rem(to, chans),
                c == chans - 1 if k == 0 else None,
            )

    def keep_own(src, dst, n, size, ch):
        own = block(c, ch)
        for i in range(size):
            dst[n, i + 1, own] = src[n, c * size + i]

        @pl.when(c > 0)
        def _():
            dst[n, 0, own] = src[n, c * size - 1]

        @pl.when(c < chans - 1)
        def _():
            dst[n, size + 1, own] = src[n, (c + 1) * size]

    def wait_main(dst, n, size, ch, rsem):
        for s in range(1, chans):
            wait_on(dst.at[n, pl.ds(1, size), pl.ds(0, ch)], rsem.at[n, s])

    def wait_halo(dst, n, size, ch, rsem, sides):
        for side in sides:
            for s in range(chans):
                def arrive():
                    wait_on(dst.at[n, side * (size + 1), pl.ds(0, ch)], rsem.at[n, side, s])

                if s == 0:
                    pl.when(c == (0, chans - 1)[side])(arrive)
                else:
                    arrive()

    def by_rows(src, dst, buf, n, pitch):
        channels, height, columns = src.shape[1], src.shape[2], src.shape[3]

        def lanes(k, carry):
            col = pl.ds(pl.multiple_of(k * LANES, LANES), LANES)
            for ch in range(channels):
                buf[pl.ds(ch * pitch, height), :] = src[n, ch, :, col].astype(F32)
            for r in range(height):
                dst[n, r, :, col] = buf[pl.ds(r, channels, stride=pitch), :].astype(BF16)
            return carry

        lax.fori_loop(0, columns // LANES, lanes, 0)

    def fine_rows(n):
        pltpu.make_async_copy(fine.at[n], raw.at[n], r_sem.at[0, n]).wait()
        by_rows(raw, fsend, tmp, n, tmp.shape[0] // in_ch)

    def coarse_rows(n):
        pltpu.make_async_copy(coarse.at[n], craw.at[n], r_sem.at[1, n]).wait()
        by_rows(craw, csend, ctmp, n, ctmp.shape[0] // c_ch)

    pl.semaphore_wait(barrier, total - 1)
    gather(lat_in, ebuf, e_send.at[0], e_recv.at[0])
    for k, par in enumerate((par0, par1, par2, par3, par4)):
        gather(par, pbuf.at[k], e_send.at[k + 1], e_recv.at[k + 1])
    weights_across(conv_in, wbuf, w_send.at[0], w_recv.at[0])
    for n in range(images):
        fine_rows(n)
        main_rows(fsend, feats, n, rows, in_ch, f_send, f_recv)
    top_rows(fsend, feats, 0, rows, in_ch, fh_send, fh_recv)
    bottom_rows(fsend, feats, 0, rows, in_ch, fh_send, fh_recv)
    for n in range(images):
        coarse_rows(n)
        keep_own(fsend, feats, n, rows, in_ch)
        keep_own(csend, level, n, c_rows, c_ch)

    local_count = float(gsize * rows * width)
    lane = lax.broadcasted_iota(jnp.int32, (D, LANES), 1)
    group = lax.broadcasted_iota(jnp.int32, (D, LANES), 0) // gsize

    def fold(x):
        acc = x[:, 0:LANES]
        for k in range(1, times):
            acc = acc + x[:, k * LANES:(k + 1) * LANES]
        return acc

    def to_row(x, slot):
        s = jnp.sum(x, axis=1, keepdims=True)
        return jnp.sum(jnp.where(lane == group + slot * GROUPS, s, 0.0), axis=0, keepdims=True)

    def from_row(row, slot):
        spread = jnp.where(lane == group + slot * GROUPS, row, 0.0)
        return jnp.sum(spread, axis=1, keepdims=True)

    def first_shift(y):
        mean = from_row(to_row(fold(y), 0), 0) / float(gsize * width)
        return jnp.broadcast_to(mean, (D, LANES))

    def stat_rows(s1, s2, shift, slot, slots):
        a = to_row(s1, slot)
        m2 = to_row(s2, slot) - a * a / local_count
        here = lax.broadcasted_iota(jnp.int32, (1, LANES), 1) // GROUPS == slot
        m2 = jnp.where(here, m2, 0.0)
        own = jnp.sum(
            jnp.where(lane == group + slot * GROUPS, shift, 0.0), axis=0, keepdims=True)
        s = a + own * (local_count / gsize)
        return s + pltpu.roll(m2, slots * GROUPS, 1)

    def exchange(row, buf, which):
        buf[0] = row

        def one(k, carry):
            to = lax.rem(me + k, total)
            pltpu.make_async_remote_copy(
                src_ref=buf.at[0], dst_ref=buf.at[k],
                send_sem=s_send.at[which], recv_sem=s_recv.at[which],
                device_id=(to // chans, lax.rem(to, chans)), device_id_type=MESH,
            ).start()
            return carry

        lax.fori_loop(1, total, one, 0)

    def combined(buf, which, slots):
        wait_on(buf.at[pl.ds(1, total - 1)], s_recv.at[which])
        parts = buf[...]
        sums = jnp.sum(parts, axis=0)
        mean = sums / pixel_count
        off = parts / local_count - mean[None]
        m2 = pltpu.roll(sums, LANES - slots * GROUPS, 1)
        var = (m2 + local_count * jnp.sum(off * off, axis=0)) / pixel_count
        inv = lax.rsqrt(var + EPS)
        return [(from_row(mean, n), from_row(inv, n)) for n in range(slots)]

    for k in range(6):
        for s in range(chans):
            wait_on((pbuf.at[k - 1] if k else ebuf).at[0], e_recv.at[k, s])
    square = (
        lax.broadcasted_iota(jnp.int32, (share, share), 0)
        == lax.broadcasted_iota(jnp.int32, (share, share), 1)
    )

    def column(k):
        return jnp.concatenate([
            jnp.sum(jnp.where(
                square, jnp.broadcast_to(pbuf[k, s].astype(F32), (share, share)), 0.0,
            ), axis=1, keepdims=True)
            for s in range(chans)
        ], axis=0)

    lat_gain, lat_shift, out_gain, out_shift, bias = (column(k) for k in range(5))
    for s in range(chans):
        wlat[s * share:(s + 1) * share, :] = ebuf[s].astype(F32).T.astype(BF16)

    src_col = lax.broadcasted_iota(jnp.int32, (half_w, width), 0)
    dst_col = lax.broadcasted_iota(jnp.int32, (half_w, width), 1)
    half = dst_col // 2
    near = jnp.where(src_col == half, 0.75, 0.0)
    other = jnp.clip(jnp.where(dst_col - 2 * half == 0, half - 1, half + 1), 0, half_w - 1)
    up[...] = (near + jnp.where(src_col == other, 0.25, 0.0)).astype(BF16)

    def lateral(features):
        return jnp.dot(wlat[...], features, preferred_element_type=F32)

    SHIFT, SCALE, OFFSET, S1, S2 = range(5)

    def centre_first(y, slot):
        coef[slot, SHIFT] = first_shift(y)
        coef[slot, S1] = jnp.zeros((D, LANES), F32)
        coef[slot, S2] = jnp.zeros((D, LANES), F32)

    def centre(y, slot):
        d = y - across(coef[slot, SHIFT], times)
        coef[slot, S1] = coef[slot, S1] + fold(d)
        coef[slot, S2] = coef[slot, S2] + fold(d * d)
        return d

    def set_norm(slot, mean, inv, gain, shift):
        scale = inv * gain
        coef[slot, SCALE] = jnp.broadcast_to(scale, (D, LANES))
        centred = jnp.broadcast_to(mean, (D, LANES)) - coef[slot, SHIFT]
        coef[slot, OFFSET] = shift - centred * scale

    row1 = jnp.zeros((1, LANES), F32)
    for n in range(images):
        wait_main(feats, n, rows, in_ch, f_recv)
        y = lateral(feats[n, 1])
        centre_first(y, n)
        lat[n, 1] = centre(y, n)

        def step(r, carry, n=n):
            lat[n, r + 1] = centre(lateral(feats[n, r + 1]), n)
            return carry

        lax.fori_loop(1, rows, step, 0)
        row1 = row1 + stat_rows(coef[n, S1], coef[n, S2], coef[n, SHIFT], n, images)
    exchange(row1, stat1, 0)
    for n in range(images):
        main_rows(csend, level, n, c_rows, c_ch, c_send, c_recv)
        top_rows(csend, level, n, c_rows, c_ch, ch_send, ch_recv)
        bottom_rows(csend, level, n, c_rows, c_ch, ch_send, ch_recv)
        if n == 0:
            weights_across(mask_in, mbuf, w_send.at[1], w_recv.at[1])
        else:
            top_rows(fsend, feats, n, rows, in_ch, fh_send, fh_recv)
            bottom_rows(fsend, feats, n, rows, in_ch, fh_send, fh_recv)
    weights_around(wbuf, w_recv.at[0], q_send.at[0], q_recv.at[0])

    edge = lax.broadcasted_iota(jnp.int32, (D, LANES), 1)

    def join(n, j, centred):
        k = j // 2
        w0, w1 = ((0.75, 0.25), (0.25, 0.75))[j % 2]
        upsampled = w0 * cols_up[k] + w1 * cols_up[k + 1]
        joined = (
            centred * across(coef[n, SCALE], times) + across(coef[n, OFFSET], times) + upsampled)
        if j == 0:
            joined = jnp.where(me > 0, joined, 0.0)
        if j == rows + 1:
            joined = jnp.where(me < total - 1, joined, 0.0)
        left = pltpu.roll(joined, 1, 1)
        right = pltpu.roll(joined, width - 1, 1)
        first = jnp.where(edge == 0, 0.0, left[:, :LANES])
        final = jnp.where(edge == LANES - 1, 0.0, right[:, width - LANES:])
        left = jnp.concatenate([first, left[:, LANES:]], axis=1)
        right = jnp.concatenate([right[:, :width - LANES], final], axis=1)
        base = j * 3 * D
        stacked[base:base + D] = left.astype(BF16)
        stacked[base + D:base + 2 * D] = joined.astype(BF16)
        stacked[base + 2 * D:base + 3 * D] = right.astype(BF16)

    for n in range(images):
        slot = images + n
        wait_main(level, n, c_rows, c_ch, c_recv)
        wait_halo(level, n, c_rows, c_ch, ch_recv, (0, 1))
        for k in range(c_rows + 2):
            cols_up[k] = jnp.dot(level[n, k], up[...], preferred_element_type=F32)

        @pl.when(me == 0)
        def _():
            cols_up[0] = cols_up[1]

        @pl.when(me == total - 1)
        def _():
            cols_up[c_rows + 1] = cols_up[c_rows]

        if n == 0:
            norms = combined(stat1, 0, images)
            for m in range(images):
                set_norm(m, norms[m][0], norms[m][1], lat_gain, lat_shift)
            wait_weights(wbuf, w_recv.at[0], q_recv.at[0])
            for k in range(9):
                wide[:, k * D:(k + 1) * D] = wbuf[k]

        def convolve(r, first=False, n=n, slot=slot):
            y = jnp.dot(
                wide[...], stacked[r * 3 * D:(r + 3) * 3 * D], preferred_element_type=F32)
            if first:
                centre_first(y, slot)
            conv[n, r] = centre(y, slot)
            if n == last:
                pltpu.make_async_copy(conv.at[n, r], last_conv.at[r], k_sem.at[r]).start()

        for j in range(1, rows + 1):
            join(n, j, lat[n, j])
        for r in range(1, rows - 1):
            convolve(r, r == 1)
        for side, j, r in ((0, 0, 0), (1, rows + 1, rows - 1)):
            wait_halo(feats, n, rows, in_ch, fh_recv, (side,))
            join(n, j, lateral(feats[n, j]) - across(coef[n, SHIFT], times))
            convolve(r, r == 0 and rows == 2)
        exchange(
            stat_rows(coef[slot, S1], coef[slot, S2], coef[slot, SHIFT], 0, 1), stat2.at[n], 1 + n)
        if n == 0:
            weights_around(mbuf, w_recv.at[1], q_send.at[1], q_recv.at[1])

    wait_weights(mbuf, w_recv.at[1], q_recv.at[1])
    pltpu.make_async_copy(mbuf.at[0], mask_out, k_sem.at[rows]).start()
    for n in range(last):
        slot = images + n
        mean, inv = combined(stat2.at[n], 1 + n, 1)[0]
        set_norm(slot, mean, inv, out_gain, out_shift)

        def finish(r, carry, n=n, slot=slot):
            rows_out[n, r] = log_softmax_row(
                conv[n, r], across(coef[slot, SCALE], times), across(coef[slot, OFFSET], times),
                mbuf[0], bias, queries[...])
            pltpu.make_async_copy(rows_out.at[n, r], done.at[n, :, r], o_sem.at[n, r]).start()
            return carry

        lax.fori_loop(0, rows, finish, 0)

    slot = images + last
    mean, inv = combined(stat2.at[last], 1 + last, 1)[0]
    set_norm(slot, mean, inv, out_gain, out_shift)
    coef[slot, SHIFT] = jnp.broadcast_to(bias, (D, LANES))
    pltpu.make_async_copy(
        coef.at[slot, pl.ds(0, 3)], last_coef, k_sem.at[rows + 1]).start()

    for which in range(1 + images):
        buf = stat1 if which == 0 else stat2.at[which - 1]
        wait_on(buf.at[pl.ds(1, total - 1)], s_send.at[which])
    for remote, only in sends:
        if only is None:
            remote().wait_send()
        else:
            @pl.when(only)
            def _():
                remote().wait_send()
    for n in range(last):
        for r in range(rows):
            pltpu.make_async_copy(rows_out.at[n, r], done.at[n, :, r], o_sem.at[n, r]).wait()
    for r in range(rows):
        pltpu.make_async_copy(conv.at[last, r], last_conv.at[r], k_sem.at[r]).wait()
    pltpu.make_async_copy(mbuf.at[0], mask_out, k_sem.at[rows]).wait()
    pltpu.make_async_copy(coef.at[slot, pl.ds(0, 3)], last_coef, k_sem.at[rows + 1]).wait()


def tail(
    done, conv, coef_in, mask_in, queries_in, out,
    rows_in, whole, rows_out, coef, mask, queries, c_sem, d_sem, o_sem, i_sem,
):
    rows, _, width = conv.shape
    last = out.shape[0] - 1
    times = width // LANES
    small = [(coef_in, coef), (mask_in, mask), (queries_in, queries)]
    for k, (src, dst) in enumerate(small):
        pltpu.make_async_copy(src, dst, i_sem.at[k]).start()
    for r in range(rows):
        pltpu.make_async_copy(conv.at[r], rows_in.at[r], c_sem.at[r]).start()
    for n in range(last):
        pltpu.make_async_copy(done.at[n], whole.at[n], d_sem.at[0, n]).start()
    for k, (src, dst) in enumerate(small):
        pltpu.make_async_copy(src, dst, i_sem.at[k]).wait()
    for r in range(rows):
        pltpu.make_async_copy(conv.at[r], rows_in.at[r], c_sem.at[r]).wait()
        rows_out[r] = log_softmax_row(
            rows_in[r], across(coef[1], times), across(coef[2], times),
            mask[...], across(coef[0], times), queries[...])
        pltpu.make_async_copy(rows_out.at[r], out.at[last, :, r], o_sem.at[r]).start()
        if r == 0:
            for n in range(last):
                pltpu.make_async_copy(done.at[n], whole.at[n], d_sem.at[0, n]).wait()
                pltpu.make_async_copy(whole.at[n], out.at[n], d_sem.at[1, n]).start()
    for n in range(last):
        pltpu.make_async_copy(whole.at[n], out.at[n], d_sem.at[1, n]).wait()
    for r in range(rows):
        pltpu.make_async_copy(rows_out.at[r], out.at[last, :, r], o_sem.at[r]).wait()


def banded(
    bands, chans,
    fine, coarse, lat_weight, lat_gain, lat_shift, out_weight, out_gain, out_shift,
    mask_weight, mask_bias, queries,
):
    images, in_ch, band_rows, width = fine.shape
    share = lat_weight.shape[0]
    c_ch, c_band = coarse.shape[1], coarse.shape[2]
    rows, c_rows = band_rows // chans, c_band // chans
    query_count = queries.shape[0]
    pixel_count = float(D // GROUPS * band_rows * bands * width)
    params = [v.reshape(1, share) for v in (lat_gain, lat_shift, out_gain, out_shift, mask_bias)]
    anywhere = pl.BlockSpec(memory_space=pl.ANY)
    vmem = pl.BlockSpec(memory_space=pltpu.VMEM)
    dma = pltpu.SemaphoreType.DMA
    before = max(images - 1, 1)
    pitch = band_rows + 1 - band_rows % 2
    c_pitch = c_band
    done, conv, coef, mask = pl.pallas_call(
        functools.partial(kernel, bands, chans, pixel_count),
        out_shape=[
            jax.ShapeDtypeStruct((before, query_count, rows, width), F32),
            jax.ShapeDtypeStruct((rows, D, width), F32),
            jax.ShapeDtypeStruct((3, D, LANES), F32),
            jax.ShapeDtypeStruct((D, D), BF16),
        ],
        in_specs=[anywhere] * 10 + [vmem],
        out_specs=[anywhere] * 4,
        scratch_shapes=[
            pltpu.VMEM((images, in_ch, band_rows, width), BF16),
            pltpu.VMEM((images, c_ch, c_band, width // 2), BF16),
            pltpu.VMEM((in_ch * pitch, LANES), F32),
            pltpu.VMEM((c_ch * c_pitch, LANES), F32),
            pltpu.VMEM((images, band_rows, in_ch, width), BF16),
            pltpu.VMEM((images, c_band, c_ch, width // 2), BF16),
            pltpu.VMEM((width // 2, width), BF16),
            pltpu.VMEM((images, rows + 2, chans * in_ch, width), BF16),
            pltpu.VMEM((images, c_rows + 2, chans * c_ch, width // 2), BF16),
            pltpu.VMEM((chans, chans * in_ch, share), BF16),
            pltpu.VMEM((5, chans, 1, share), BF16),
            pltpu.VMEM((9, D, D), BF16),
            pltpu.VMEM((1, D, D), BF16),
            pltpu.VMEM((D, chans * in_ch), BF16),
            pltpu.VMEM((D, 9 * D), BF16),
            pltpu.VMEM((images, rows + 2, D, width), F32),
            pltpu.VMEM((c_rows + 2, D, width), F32),
            pltpu.VMEM(((rows + 2) * 3 * D, width), BF16),
            pltpu.VMEM((images, rows, D, width), F32),
            pltpu.VMEM((before, rows, query_count, width), F32),
            pltpu.VMEM((2 * images, 5, D, LANES), F32),
            pltpu.VMEM((bands * chans, 1, LANES), F32),
            pltpu.VMEM((images, bands * chans, 1, LANES), F32),
            dma((2, images)),
            dma((images, chans)), dma((images, chans)),
            dma((images, 2, chans)), dma((images, 2, chans)),
            dma((images, chans)), dma((images, chans)),
            dma((images, 2, chans)), dma((images, 2, chans)),
            dma((6, chans)), dma((6, chans)), dma((2, chans)), dma((2, chans)),
            dma((2, chans, 4)), dma((2, chans, 4)),
            dma((1 + images,)), dma((1 + images,)),
            dma((before, rows)), dma((rows + 2,)),
        ],
        compiler_params=pltpu.CompilerParams(
            has_side_effects=True, collective_id=0, vmem_limit_bytes=60 * 1024 * 1024),
    )(
        fine, coarse, lat_weight.T, *params, out_weight.reshape(9, share, D), mask_weight[None],
        queries,
    )
    return pl.pallas_call(
        tail,
        out_shape=jax.ShapeDtypeStruct((images, query_count, rows, width), F32),
        in_specs=[anywhere] * 5,
        out_specs=anywhere,
        scratch_shapes=[
            pltpu.VMEM((rows, D, width), F32),
            pltpu.VMEM((before, query_count, rows, width), F32),
            pltpu.VMEM((rows, query_count, width), F32),
            pltpu.VMEM((3, D, LANES), F32),
            pltpu.VMEM((D, D), BF16),
            pltpu.VMEM((query_count, D), BF16),
            dma((rows,)), dma((2, before)), dma((rows,)), dma((3,)),
        ],
        compiler_params=pltpu.CompilerParams(vmem_limit_bytes=60 * 1024 * 1024),
    )(done, conv, coef, mask, queries)


def gathered(
    bands, chans,
    fine, coarse, lat_weight, lat_gain, lat_shift, out_weight, out_gain, out_shift,
    mask_weight, mask_bias, queries,
):
    def whole(x, axis):
        return lax.all_gather(x, "chan", axis=axis, tiled=True)

    fine, coarse = whole(fine, 1), whole(coarse, 1)
    lat_weight, mask_weight = whole(lat_weight, 0), whole(mask_weight, 0)
    out_weight = whole(out_weight, 2)
    lat_gain, lat_shift, out_gain, out_shift, mask_bias = (
        whole(v, 0).astype(F32)[None, :, None, None]
        for v in (lat_gain, lat_shift, out_gain, out_shift, mask_bias))
    images, _, band_rows, width = fine.shape
    c_band, half_w = coarse.shape[2], coarse.shape[3]
    rows = band_rows // chans
    b = lax.axis_index("band")
    count = float(D // GROUPS * band_rows * bands * width)

    def norm(x, gain, shift, over):
        grouped = x.reshape(images, GROUPS, -1)
        mean = lax.psum(jnp.sum(grouped, axis=2), over) / count
        off = grouped - mean[:, :, None]
        var = lax.psum(jnp.sum(off * off, axis=2), over) / count
        y = (off * lax.rsqrt(var + EPS)[:, :, None]).reshape(x.shape)
        return y * gain + shift

    def with_border(x, clamp):
        n = x.shape[2]
        down = [(k, (k + 1) % bands) for k in range(bands)]
        upward = [((k + 1) % bands, k) for k in range(bands)]
        above = lax.ppermute(x[:, :, n - 1:], "band", down)
        below = lax.ppermute(x[:, :, :1], "band", upward)
        above = jnp.where(b == 0, x[:, :, :1] if clamp else jnp.zeros_like(above), above)
        below = jnp.where(
            b == bands - 1, x[:, :, n - 1:] if clamp else jnp.zeros_like(below), below)
        return jnp.concatenate([above, x, below], axis=2)

    def doubled(x, axis):
        n = x.shape[axis] - 2
        low, mid, high = (lax.slice_in_dim(x, k, k + n, axis=axis) for k in range(3))
        pair = jnp.stack([0.25 * low + 0.75 * mid, 0.75 * mid + 0.25 * high], axis + 1)
        return pair.reshape(x.shape[:axis] + (2 * n,) + x.shape[axis + 1:])

    def mix(w, x):
        return jnp.einsum("oi,nirc->norc", w, x, preferred_element_type=F32)

    lateral = norm(mix(lat_weight, fine), lat_gain, lat_shift, "band")
    tall = doubled(with_border(coarse, True).astype(F32), 2)
    upsampled = doubled(jnp.pad(tall, ((0, 0), (0, 0), (0, 0), (1, 1)), mode="edge"), 3)
    joined = (lateral + upsampled).astype(BF16)
    padded = lax.dynamic_slice_in_dim(
        with_border(joined, False), lax.axis_index("chan") * rows, rows + 2, axis=2)
    padded = jnp.pad(padded, ((0, 0), (0, 0), (0, 0), (1, 1)))
    conv = sum(
        mix(out_weight[a, t], padded[:, :, a:a + rows, t:t + width])
        for a in range(3) for t in range(3))
    act = jnp.maximum(norm(conv, out_gain, out_shift, ("band", "chan")), 0.0).astype(BF16)
    features = (mix(mask_weight, act) + mask_bias).astype(BF16)
    logits = mix(queries, features)
    shifted = logits - jnp.max(logits, axis=1, keepdims=True)
    return shifted - jnp.log(jnp.sum(jnp.exp(shifted), axis=1, keepdims=True))


def per_device(bands, chans, fine, coarse, *rest):
    thick = coarse.shape[2] % chans == 0 and fine.shape[2] == 2 * coarse.shape[2]
    return (banded if thick else gathered)(bands, chans, fine, coarse, *rest)


def solution(mesh):
    return jax.shard_map(
        functools.partial(per_device, mesh.shape["band"], mesh.shape["chan"]),
        mesh=mesh,
        in_specs=(
            P(None, "chan", "band", None),
            P(None, "chan", "band", None),
            P("chan", None),
            P("chan"),
            P("chan"),
            P(None, None, "chan", None),
            P("chan"),
            P("chan"),
            P("chan", None),
            P("chan"),
            P(),
        ),
        out_specs=P(None, None, ("band", "chan"), None),
        check_vma=False,
    )
```
